32 devices in a mesh: site: 2 (over y), owner: 16 (over z, x, core).
Axes of the slice: x: 2, y: 2, z: 4, core: 2. Of those that a mesh axis runs over, the one named last changes fastest.
Arguments:
- green_tensor: bfloat16 [4096, 6, 1024], P(('site', 'owner')), parts along dimension 0, may hold values from -6 to 6
- mechanism: float32 [2, 6, 2048], P(None, None, 'owner'), may hold values from -2.5 to 2.5
- point_owner: int32 [16, 128, 1], P('owner'), may hold values from 0 to 15; in each aligned block of 128 rows (0 to 127, 128 to 255, ..., all dimensions but the last counted through in order) at most 16 rows name the same one
- point_row: int32 [16, 128], P('owner'), may hold values from 0 to 127
- onset_step: int32 [16, 128], P('owner'), may hold values from 0 to 511
- slip_amount: float32 [16, 128], P('owner'), may hold values from 0.01 to 0.1
- point_count: int32 [16], P('owner'), may hold values from 12 to 128
- rake_angle: float32 [16], P('owner'), may hold values from -3.140625 to 3.140625
- slip_rate: float32 [16, 64], P('owner'), may hold values from 0.02 to 0.2
Outputs:
- seismogram: float32 [32, 1024], P(('site', 'owner')), parts along dimension 0
The draws below stay inside these ranges and needn't reach their ends.
There are 2 independent parts, one for each index of `site`. The reference program is written for one: setup_inputs(seed, part) draws one part's arguments, and reference() takes and returns one part's arrays. A program takes and returns all parts, laid end to end along the dimension named above; an argument that names none is the same for every part. Nothing has to cross between parts.
Inputs may be any that keep to these rules, and one draw needn't show every extreme that they name: `point_owner`: among the 128 entries of one device's variations, at most 16 name the same owner, a bound that some block reaches of them.
All inputs are finite; a program needn't handle non-finite values.
Results may differ from the reference program's by a relative error of at most 0.0029.
Values may be sent and summed in bfloat16 or wider, within the bound.
A program may use at most 64 MiB of HBM per device.

```python
import math
import jax
import jax.numpy as jnp
import numpy as np
from jax import lax

T_SIZE = 1024
K = 64
P_DEV = 128
V_DEV = 1
LMAX = 128
POINTS = 2048
VARS = 16
OMAX = 512
CAP = 16
N_OWNER = 16


def set_ends(values, rng, least, high):
    longest = values.shape.index(max(values.shape))
    spots = []
    for shift in (0, 1):
        where = [jax.random.randint(jax.random.fold_in(rng, axis), (), 0, length) for axis, length in enumerate(values.shape)]
        where[longest] = (where[longest] + shift) % values.shape[longest]
        spots.append(tuple(where))
    return values.at[spots[0]].set(least).at[spots[1]].set(high)


def block_levels(key, extent, split, least, high):
    def one(dim, blocks):
        heights = jax.random.uniform(jax.random.fold_in(jax.random.fold_in(key, 6), dim), (blocks,), jnp.float32, least / len(split), high / len(split))
        return jnp.repeat(jnp.exp(heights), extent[dim] // blocks).reshape((-1,) + (1,) * (len(extent) - dim - 1))

    factor_of = one(*split[0])
    for cut in split[1:]:
        factor_of = factor_of * one(*cut)
    return factor_of


def routed_block(own_key, own, number, rows, number_of, top, limit, skew):
    sequence = jax.random.permutation(own_key, number_of)
    heavy_load, usual = load_shares(number_of, rows * top, limit, skew, True), load_shares(number_of, rows * top, limit, skew, False)
    places = jnp.arange(number_of)

    def named(tallies, rotation):
        used = int((tallies > 0).sum())
        fixed = max(1, used // 4)
        passed = fixed + (places - fixed + rotation * (used - fixed)) % max(1, number_of - fixed)
        return jnp.zeros((number_of,), jnp.int32).at[sequence[jnp.where(places < fixed, places, passed)]].set(jnp.asarray(tallies, jnp.int32))

    tallies = jnp.where(number % 4 == 0, named(heavy_load, number // 4), named(usual, number - number // 4 - 1))
    mixed = jax.random.permutation(jax.random.fold_in(own, 3), number_of)
    donor, sink = mixed[0:number_of // 2 * 2:2], mixed[1:number_of // 2 * 2:2]
    slack = jnp.minimum(tallies[donor] - 1, limit - tallies[sink]) // 2
    slack = jnp.where((donor == sequence[0]) | (sink == sequence[0]) | (tallies[sink] == 0), 0, jnp.maximum(slack, 0))
    passed = jax.random.randint(jax.random.fold_in(own, 4), (number_of // 2,), 0, 1 << 20) % (slack + 1)
    tallies = tallies.at[donor].add(-passed).at[sink].add(passed)
    members = jnp.searchsorted(jnp.cumsum(tallies), jnp.arange(rows * top), side="right").astype(jnp.int32)
    table = members.reshape(top, rows).T
    table = table[jax.random.permutation(jax.random.fold_in(own, 1), rows)]
    rotation = jax.random.randint(jax.random.fold_in(own, 2), (rows, 1), 0, top)
    return jnp.take_along_axis(table, (jnp.arange(top)[None, :] + rotation) % top, axis=1)


def load_shares(count, total, reach, skew, full):
    weights = [(1 << 20) // math.isqrt(standing ** skew) + 1 for standing in range(1, count + 1)]
    largest = reach if full else min(reach, max(-(-total // count), total * weights[0] // sum(weights)))
    least = 1 if total - largest >= count - 1 else 0
    given, rest = [largest] + [least] * (count - 1), total - largest - least * (count - 1)
    while rest > 0:
        candidates = [i for i in range(1, count) if given[i] < largest] or [i for i in range(1, count) if given[i] < reach]
        pool, budget = sum([weights[i] for i in candidates]), rest
        for i in candidates:
            addition = min(reach - given[i], max(1, budget * weights[i] // pool), rest)
            given[i] = given[i] + addition
            rest = rest - addition
    return np.array(given)


def noise(rng, dims, scale, limit, cuts=(), held_as=jnp.bfloat16):
    entries = jax.random.normal(rng, dims, jnp.float32) * scale
    if len(cuts) > 0:
        entries = block_levels(rng, dims, cuts, -0.22, 0.18) * entries
    return jnp.clip(entries, min=-limit, max=limit).astype(held_as)


def setup_inputs(seed: int = 0, part: int = 0) -> dict:
    splits = jax.random.split(jax.random.key(seed), 10)
    part_keys = jax.random.split(jax.random.fold_in(splits[9], part), 10)
    green_tensor = noise(part_keys[0], (POINTS, 6, T_SIZE), 1.0, 6.0, ((0, 16),))
    mechanism = noise(splits[1], (2, 6, POINTS), 6 ** -0.5, 2.5, ((2, 16),), jnp.float32)
    point_owner_keys = jax.random.split(jax.random.fold_in(splits[2], 1), VARS * LMAX // (V_DEV * LMAX))
    point_owner_turns = jax.random.permutation(jax.random.fold_in(splits[2], 3), VARS * LMAX // (V_DEV * LMAX))
    point_owner = jax.vmap(lambda own, number: routed_block(jax.random.fold_in(splits[2], 2), own, number, V_DEV * LMAX, N_OWNER, 1, CAP, 2))(point_owner_keys, point_owner_turns).reshape((VARS, LMAX, 1))
    point_row = set_ends(jax.random.randint(splits[3], (VARS, LMAX), 0, P_DEV), jax.random.fold_in(splits[3], 1), 0, P_DEV - 1).astype(jnp.int32)
    onset_step = set_ends(jax.random.randint(splits[4], (VARS, LMAX), 0, OMAX), jax.random.fold_in(splits[4], 1), 0, OMAX - 1).astype(jnp.int32)
    slip_amount = jnp.clip(jnp.exp(math.log(0.1) - 2.3025851 * jax.random.uniform(splits[5], (VARS, LMAX), jnp.float32) ** block_levels(splits[5], (VARS, LMAX), ((0, 16),), -0.2, 0.2)), 0.01, 0.1)
    point_count = set_ends(jax.random.randint(splits[6], (VARS,), LMAX // 10, LMAX + 1), jax.random.fold_in(splits[6], 1), LMAX // 10, LMAX).astype(jnp.int32)
    rake_angle = jnp.clip(jax.random.uniform(splits[7], (VARS,), jnp.float32, -3.140625, 3.140625), -3.140625, 3.140625)
    slip_rate = jnp.clip(jnp.exp(math.log(0.2) - 2.3025851 * jax.random.uniform(splits[8], (VARS, K), jnp.float32) ** block_levels(splits[8], (VARS, K), ((0, 16),), -0.2, 0.2)), 0.02, 0.2)
    return {"green_tensor": green_tensor, "mechanism": mechanism, "point_owner": point_owner, "point_row": point_row, "onset_step": onset_step, "slip_amount": slip_amount, "point_count": point_count, "rake_angle": rake_angle, "slip_rate": slip_rate}


def delay_traces(traces, steps):
    length = traces.shape[-1]
    source_step = jnp.arange(length, dtype=jnp.int32) - steps[..., None]
    inside = source_step >= 0
    time_index = jnp.broadcast_to(jnp.maximum(source_step, 0)[..., None, :], traces.shape)
    moved = jnp.take_along_axis(traces, time_index, axis=-1)
    return jnp.where(inside[..., None, :], moved, jnp.zeros_like(moved))


def smooth(signal, kernel):
    taps = kernel.shape[1]
    filtered = lax.conv_general_dilated(signal[None], kernel[:, None, ::-1], (1,), ((taps - 1, 0),), dimension_numbers=("NCH", "OIH", "NCH"), feature_group_count=signal.shape[0], precision=lax.Precision.HIGHEST)
    return filtered[0]


def project(green_block, mech_block):
    return jnp.einsum("kcp,pct->pkt", mech_block, green_block.astype(jnp.float32), precision=lax.Precision.HIGHEST).astype(jnp.bfloat16)


def coefficients(slip_amount, point_count, rake_angle):
    length = slip_amount.shape[1]
    alive_mask = jnp.arange(length, dtype=jnp.int32)[None, :] < point_count[:, None]
    weight = jnp.where(alive_mask, slip_amount, jnp.zeros_like(slip_amount))
    return jnp.stack([jnp.cos(rake_angle)[:, None] * weight, jnp.sin(rake_angle)[:, None] * weight], axis=2)


def reference(green_tensor, mechanism, point_owner, point_row, onset_step, slip_amount, point_count, rake_angle, slip_rate):
    def project_pair(pair):
        return project(pair[0], pair[1])

    blocks = lax.map(project_pair, (green_tensor.reshape(N_OWNER, P_DEV, 6, T_SIZE), jnp.transpose(mechanism.reshape(2, 6, N_OWNER, P_DEV), (2, 0, 1, 3))))
    traces = blocks.reshape(N_OWNER * P_DEV, 2, T_SIZE)
    coefficient = coefficients(slip_amount, point_count, rake_angle)
    point_index = (point_owner[:, :, 0] * P_DEV + point_row).astype(jnp.int32)

    def one_variation(items):
        index_row, delay_row, coef_row = items
        shifted = delay_traces(traces[index_row], delay_row)
        return jnp.sum(shifted.astype(jnp.float32) * coef_row[:, :, None], axis=(0, 1))

    summed = lax.map(one_variation, (point_index, onset_step, coefficient))
    return smooth(summed, slip_rate)
```

```python
import functools

import jax
import jax.numpy as jnp
from jax import lax
from jax.experimental import pallas as pl
from jax.experimental.pallas import tpu as pltpu
from jax.sharding import PartitionSpec as P

MESH = pl.DeviceIdType.MESH
LANES = 128
GROUP = 32
TILE = 16
SCALE = 2.0**34
STORE_LIMIT = 1 << 20


def iota(shape, axis):
    return lax.broadcasted_iota(jnp.int32, shape, axis)


def kernel(
    n,
    cap,
    green_hbm,
    mech_hbm,
    owner_hbm,
    row_hbm,
    onset_hbm,
    slip_hbm,
    count_hbm,
    rake_hbm,
    rate_hbm,
    out_ref,
    green,
    mech_ref,
    owner_ref,
    row_ref,
    onset_ref,
    slip_ref,
    count_ref,
    rake_ref,
    rate_ref,
    mech,
    traces,
    ask,
    use,
    part,
    parts,
    load_sem,
    small_sem,
    own_sem,
    ask_send,
    ask_recv,
    part_send,
    part_recv,
):
    me = lax.axis_index("owner")
    comps, points, length = green_hbm.shape
    blocks = length // LANES
    stride = 2 * blocks + 1
    entries = row_ref.shape[1]
    taps = rate_ref.shape[1]
    groups = points // GROUP

    def peer(d):
        return d + jnp.where(d >= me, 1, 0)

    barrier = pltpu.get_barrier_semaphore()

    @pl.loop(0, n - 1)
    def _(d):
        pl.semaphore_signal(barrier, inc=1, device_id={"owner": peer(d)}, device_id_type=MESH)

    smalls = [
        pltpu.make_async_copy(source, target, small_sem.at[i])
        for i, (source, target) in enumerate(
            [
                (owner_hbm, owner_ref),
                (row_hbm, row_ref),
                (onset_hbm, onset_ref),
                (slip_hbm, slip_ref),
                (count_hbm, count_ref),
                (rake_hbm, rake_ref),
                (mech_hbm, mech_ref),
                (rate_hbm, rate_ref),
            ]
        )
    ]
    for small in smalls:
        small.start()
    loads = [
        pltpu.make_async_copy(
            green_hbm.at[:, pl.ds(g * GROUP, GROUP)],
            green.at[:, pl.ds(g * GROUP, GROUP)],
            load_sem.at[g],
        )
        for g in range(groups)
    ]
    for load in loads:
        load.start()
    for small in smalls:
        small.wait()

    alive = iota((1, entries), 1) < count_ref[0, 0]
    weight = jnp.where(alive, slip_ref[...], 0.0)
    rake = jnp.full((1, entries), rake_ref[0, 0], jnp.float32)
    named = owner_ref[...] == iota((n, entries), 0)
    one_hot = named.astype(jnp.float32)
    before = (iota((entries, entries), 0) < iota((entries, entries), 1)).astype(jnp.bfloat16)
    ahead = jnp.dot(one_hot.astype(jnp.bfloat16), before, preferred_element_type=jnp.float32)
    rank = jnp.sum(one_hot * ahead, axis=0, keepdims=True)
    place = (rank == iota((LANES, entries), 0).astype(jnp.float32)).astype(jnp.float32)
    fields = jnp.concatenate(
        [
            one_hot * row_ref[...].astype(jnp.float32),
            one_hot * onset_ref[...].astype(jnp.float32),
            one_hot * (jnp.cos(rake) * weight),
            one_hot * (jnp.sin(rake) * weight),
        ],
        axis=0,
    )
    slots = lax.dot_general(
        fields,
        place,
        (((1,), (1,)), ((), ())),
        precision=lax.Precision.HIGHEST,
        preferred_element_type=jnp.float32,
    )
    rows = jnp.clip((slots[:n] + 0.5).astype(jnp.int32), 0, points - 1)
    onsets = jnp.clip((slots[n : 2 * n] + 0.5).astype(jnp.int32), 0, length - 1)
    fixed = (slots[2 * n :] * SCALE).astype(jnp.int32)
    lanes = iota((n, LANES), 1)
    table = jnp.where(lanes < cap, rows, pltpu.roll(onsets, cap, 1))
    table = jnp.where(lanes < 2 * cap, table, pltpu.roll(fixed[:n], 2 * cap, 1))
    table = jnp.where(lanes < 3 * cap, table, pltpu.roll(fixed[n:], 3 * cap, 1))
    ask[...] = table.reshape(n, 1, LANES)

    def ask_copy(d):
        to = peer(d)
        return pltpu.make_async_remote_copy(
            src_ref=ask.at[to],
            dst_ref=use.at[me],
            send_sem=ask_send.at[to],
            recv_sem=ask_recv.at[me],
            device_id={"owner": to},
            device_id_type=MESH,
        )

    pl.semaphore_wait(barrier, n - 1)

    @pl.loop(0, n - 1)
    def _(d):
        ask_copy(n - 2 - d).start()

    own_down = pltpu.make_async_copy(ask.at[me], use.at[me], own_sem)
    own_down.start()

    traces[...] = jnp.zeros_like(traces)
    for c in range(comps):
        mech[pl.ds(2 * c, 2), :] = mech_ref[c]
    factor = mech[...].T
    for g in range(groups):
        loads[g].wait()
        for low in range(g * GROUP, (g + 1) * GROUP, TILE):
            part_of = factor[low : low + TILE]
            scale = [
                jnp.broadcast_to(part_of[:, i : i + 1], (TILE, LANES)) for i in range(2 * comps)
            ]
            for s in range(blocks):
                tiles = [
                    green[c, pl.ds(low, TILE), pl.ds(s * LANES, LANES)].astype(jnp.float32)
                    for c in range(comps)
                ]
                for k in range(2):
                    value = sum(tiles[c] * scale[2 * c + k] for c in range(comps))
                    start = (k * points + low) * stride + blocks + s
                    traces[pl.ds(start, TILE, stride=stride), :] = value.astype(
                        jnp.bfloat16
                    ).astype(jnp.float32)

    lane = iota((blocks, LANES), 1)

    def partial_sum(v):
        total = jnp.zeros((blocks, LANES), jnp.float32)
        for j in range(cap):
            row, onset, first, second = (use[v, 0, i * cap + j] for i in range(4))
            first, second = first.astype(jnp.float32), second.astype(jnp.float32)
            low = onset & (LANES - 1)
            start = row * stride + blocks - (onset >> (LANES.bit_length() - 1))
            other = start + points * stride
            same = (
                first * traces[pl.ds(start, blocks), :] + second * traces[pl.ds(other, blocks), :]
            )
            prior = (
                first * traces[pl.ds(start - 1, blocks), :]
                + second * traces[pl.ds(other - 1, blocks), :]
            )
            total += pltpu.roll(jnp.where(lane >= LANES - low, prior, same), low, 1)
        return total * (1.0 / SCALE)

    def part_copy(d):
        to = peer(d)
        return pltpu.make_async_remote_copy(
            src_ref=part.at[to],
            dst_ref=parts.at[me],
            send_sem=part_send.at[to],
            recv_sem=part_recv.at[me],
            device_id={"owner": to},
            device_id_type=MESH,
        )

    @pl.loop(0, n - 1)
    def _(d):
        to = peer(d)
        pltpu.make_async_copy(use.at[to], use.at[to], ask_recv.at[to]).wait()
        part[to] = partial_sum(to)
        part_copy(d).start()

    own_down.wait()
    own = partial_sum(me)

    def gather(d, total):
        source = peer(d)
        pltpu.make_async_copy(parts.at[source], parts.at[source], part_recv.at[source]).wait()
        return total + parts[source]

    summed = lax.fori_loop(0, n - 1, gather, own)

    above = jnp.where(iota((blocks, LANES), 0) == 0, 0.0, pltpu.roll(summed, 1, 0))
    result = summed * rate_ref[0, 0]
    for j in range(1, taps):
        result += pltpu.roll(jnp.where(lane >= LANES - j, above, summed), j, 1) * rate_ref[0, j]
    out_ref[...] = result

    @pl.loop(0, n - 1)
    def _(d):
        ask_copy(d).wait_send()
        part_copy(d).wait_send()


def store(value_ref, out_ref, sem):
    copy = pltpu.make_async_copy(value_ref, out_ref, sem)
    copy.start()
    copy.wait()


def local(
    green_tensor,
    mechanism,
    point_owner,
    point_row,
    onset_step,
    slip_amount,
    point_count,
    rake_angle,
    slip_rate,
):
    n = lax.axis_size("owner")
    variations, entries = point_row.shape
    assert variations == 1
    cap = 2 * entries // n
    points, comps, length = green_tensor.shape
    blocks = length // LANES
    hbm = pl.BlockSpec(memory_space=pltpu.HBM)
    vmem = pl.BlockSpec(memory_space=pltpu.VMEM)
    out = pl.pallas_call(
        functools.partial(kernel, n, cap),
        out_shape=pltpu.VMEM((blocks, LANES), jnp.float32),
        in_specs=[hbm] * 9,
        out_specs=vmem,
        scratch_shapes=[
            pltpu.VMEM((comps, points, length), jnp.bfloat16),
            pltpu.VMEM((comps, 2, points), jnp.float32),
            pltpu.VMEM((1, entries), jnp.int32),
            pltpu.VMEM((1, entries), jnp.int32),
            pltpu.VMEM((1, entries), jnp.int32),
            pltpu.VMEM((1, entries), jnp.float32),
            pltpu.SMEM((1, 1), jnp.int32),
            pltpu.SMEM((1, 1), jnp.float32),
            pltpu.SMEM(slip_rate.shape, jnp.float32),
            pltpu.VMEM((LANES, points), jnp.float32),
            pltpu.VMEM(((2 * points + 1) * (2 * blocks + 1), LANES), jnp.float32),
            pltpu.VMEM((n, 1, LANES), jnp.int32),
            pltpu.SMEM((n, 1, LANES), jnp.int32),
            pltpu.VMEM((n, blocks, LANES), jnp.float32),
            pltpu.VMEM((n, blocks, LANES), jnp.float32),
            pltpu.SemaphoreType.DMA((points // GROUP,)),
            pltpu.SemaphoreType.DMA((8,)),
            pltpu.SemaphoreType.DMA,
            pltpu.SemaphoreType.DMA((n,)),
            pltpu.SemaphoreType.DMA((n,)),
            pltpu.SemaphoreType.DMA((n,)),
            pltpu.SemaphoreType.DMA((n,)),
        ],
        compiler_params=pltpu.CompilerParams(
            collective_id=0, has_side_effects=True
        ),
        name="seismogram",
    )(
        green_tensor.transpose(1, 0, 2),
        mechanism.transpose(1, 0, 2),
        point_owner.reshape(1, entries),
        point_row,
        onset_step,
        slip_amount,
        point_count.reshape(1, 1),
        rake_angle.reshape(1, 1),
        slip_rate,
    )
    result = pl.pallas_call(
        store,
        out_shape=jax.ShapeDtypeStruct((blocks, LANES), jnp.float32),
        in_specs=[vmem],
        out_specs=pl.BlockSpec(memory_space=pl.ANY),
        scratch_shapes=[pltpu.SemaphoreType.DMA],
        compiler_params=pltpu.CompilerParams(vmem_limit_bytes=STORE_LIMIT),
        name="store",
    )(out)
    return result.reshape(1, length)


def solution(mesh):
    in_specs = (
        P(("site", "owner"), None, None),
        P(None, None, "owner"),
        P("owner", None, None),
        P("owner", None),
        P("owner", None),
        P("owner", None),
        P("owner"),
        P("owner"),
        P("owner", None),
    )
    out_specs = P(("site", "owner"), None)
    return jax.shard_map(local, mesh=mesh, in_specs=in_specs, out_specs=out_specs, check_vma=False)
```
